32 devices in a mesh: gx: 2 (over x), gy: 2 (over core), gz: 8 (over z, y).
Axes of the slice: x: 2, y: 2, z: 4, core: 2. Of those that a mesh axis runs over, the one named last changes fastest.
Arguments:
- state_re: float32 [33554432], P(('gx', 'gy', 'gz')), may hold values from -6 to 6
- state_im: float32 [33554432], P(('gx', 'gy', 'gz')), may hold values from -6 to 6
Outputs:
- out_re: float32 [33554432], P(('gx', 'gy', 'gz'))
- out_im: float32 [33554432], P(('gx', 'gy', 'gz'))
- probability: float32 [33554432], P(('gx', 'gy', 'gz'))
The draws below stay inside these ranges and needn't reach their ends.
All inputs are finite; a program needn't handle non-finite values.
Results may differ from the reference program's by a relative error of at most 0.000071.
Values sent between devices are 32-bit elements; how exact they have to be, the bound alone decides.
No kernel may reach another device: no remote copies, remote signals or barrier semaphores. Data moves between devices by JAX's collectives and lax.ppermute only.
A program may use at most 128 MiB of HBM per device.

```python
import jax
import jax.numpy as jnp

AMPS = 1048576
NSTATE = 33554432
DEVICES = 32


def levels(key, dims, shards, smallest, top_value):
    factor_of, own = 1.0, jax.random.fold_in(key, 6)
    for dim, blocks in shards:
        draws = jnp.exp(jax.random.uniform(jax.random.fold_in(own, dim), (blocks,), jnp.float32, smallest / len(shards), top_value / len(shards)))
        factor_of = factor_of * jnp.repeat(draws, dims[dim] // blocks).reshape([-1 if axis == dim else 1 for axis in range(len(dims))])
    return factor_of


def gaussian(key, shape, deviation, reach, pieces=(), dtype=jnp.bfloat16):
    factor_of = levels(key, shape, pieces, -0.22, 0.18) if pieces else 1.0
    drawn = jax.random.normal(key, shape, jnp.float32) * deviation * factor_of
    return jnp.minimum(jnp.maximum(drawn, -reach), reach).astype(dtype)


def setup_inputs(seed: int = 0) -> dict:
    arg_keys = jax.random.split(jax.random.key(seed), 3)
    state_re = gaussian(arg_keys[0], (NSTATE,), 1.0, 6.0, ((0, 32),), jnp.float32)
    state_im = gaussian(arg_keys[1], (NSTATE,), 1.0, 6.0, ((0, 32),), jnp.float32)
    return dict(state_re=state_re, state_im=state_im)


def reverse_bits(values, nbits, total):
    shaped = values.reshape((2,) * nbits)
    return jnp.transpose(shaped, tuple(range(nbits - 1, -1, -1))).reshape(total)


def reference(state_re, state_im):
    total = AMPS * DEVICES
    nbits = total.bit_length() - 1
    state = state_re + 1j * state_im
    spectrum = jnp.fft.ifft(state, norm="ortho")
    out_re = reverse_bits(jnp.real(spectrum), nbits, total).astype(jnp.float32)
    out_im = reverse_bits(jnp.imag(spectrum), nbits, total).astype(jnp.float32)
    probability = out_re * out_re + out_im * out_im
    return out_re, out_im, probability
```

```python
import functools
import math

import jax
import jax.numpy as jnp
import numpy as np
from jax import lax
from jax.experimental import pallas as pl
from jax.experimental.pallas import tpu as pltpu
from jax.sharding import PartitionSpec as P

AXES = ("gx", "gy", "gz")
LANES = 128
CHUNKS = 2


def reversed_bits(count):
    bits = count.bit_length() - 1
    values = np.arange(count)
    result = np.zeros(count, np.int32)
    for place in range(bits):
        result += ((values >> place) & 1) << (bits - 1 - place)
    return result.astype(np.int32)


def phases(product, modulus):
    angle = (product % modulus).astype(jnp.float32) * (2.0 * math.pi / modulus)
    return jnp.cos(angle), jnp.sin(angle)


def halves(values):
    high = values.astype(jnp.bfloat16)
    low = (values - high.astype(jnp.float32)).astype(jnp.bfloat16)
    return high, low


def table_halves(values):
    high = lax.reduce_precision(values, 8, 7)
    return high.astype(jnp.bfloat16), (values - high).astype(jnp.bfloat16)


def fourier(reals, imags):
    count = len(reals)
    span = count // 2
    reals, imags = list(reals), list(imags)
    while span >= 1:
        for start in range(0, count, 2 * span):
            for offset in range(span):
                top, bottom = start + offset, start + offset + span
                ar, ai, br, bi = reals[top], imags[top], reals[bottom], imags[bottom]
                reals[top], imags[top] = ar + br, ai + bi
                dr, di = ar - br, ai - bi
                if offset == 0:
                    reals[bottom], imags[bottom] = dr, di
                elif 2 * offset == span:
                    reals[bottom], imags[bottom] = -di, dr
                else:
                    angle = math.pi * offset / span
                    c, s = math.cos(angle), math.sin(angle)
                    if 4 * offset == span:
                        reals[bottom], imags[bottom] = (dr - di) * c, (dr + di) * c
                    elif 4 * offset == 3 * span:
                        reals[bottom], imags[bottom] = -(dr + di) * s, (dr - di) * s
                    else:
                        reals[bottom], imags[bottom] = dr * c - di * s, dr * s + di * c
        span //= 2
    return reals, imags


def device_kernel(re_ref, im_ref, cos_ref, sin_ref, high_ref, low_ref):
    count = re_ref.shape[0]
    reals, imags = fourier([re_ref[d] for d in range(count)], [im_ref[d] for d in range(count)])
    for e in range(count):
        c, s = cos_ref[:, e : e + 1], sin_ref[:, e : e + 1]
        yr = reals[e] * c - imags[e] * s
        yi = reals[e] * s + imags[e] * c
        high, low = halves(yr)
        high_ref[e, :, :LANES], low_ref[e, :, :LANES] = high, low
        high, low = halves(yi)
        high_ref[e, :, LANES:], low_ref[e, :, LANES:] = high, low


def device_stage(re, im, cosine, sine):
    devices, rows, lanes = re.shape
    block = 16
    spec = pl.BlockSpec((devices, block, lanes), lambda i: (0, i, 0))
    table = pl.BlockSpec((block, devices), lambda i: (i, 0))
    out = pl.BlockSpec((devices, block, 2 * lanes), lambda i: (0, i, 0))
    shape = jax.ShapeDtypeStruct((devices, rows, 2 * lanes), jnp.bfloat16)
    return pl.pallas_call(
        device_kernel,
        grid=(rows // block,),
        in_specs=[spec, spec, table, table],
        out_specs=[out, out],
        out_shape=[shape, shape],
        cost_estimate=pl.CostEstimate(
            flops=80 * devices * rows * lanes, bytes_accessed=16 * devices * rows * lanes, transcendentals=0
        ),
        name="device_stage",
    )(re, im, cosine, sine)


def row_kernel(high_ref, low_ref, table_ref, out_ref):
    rows = table_ref.shape[1] // 2
    dot = functools.partial(jnp.dot, preferred_element_type=jnp.float32)
    high, low = high_ref[0], low_ref[0]
    mixed = dot(table_ref[0], high) + dot(table_ref[1], high) + dot(table_ref[0], low)
    out_ref[0, :rows] = mixed[:rows, :LANES] - mixed[rows:, LANES:]
    out_ref[0, rows:] = mixed[rows:, :LANES] + mixed[:rows, LANES:]


def row_stage(high, low, table):
    devices, rows, wide = high.shape
    part = table.shape[1]
    spec = pl.BlockSpec((1, rows, wide), lambda e: (e, 0, 0))
    return pl.pallas_call(
        row_kernel,
        grid=(devices,),
        in_specs=[spec, spec, pl.BlockSpec((2, part, rows), lambda e: (0, 0, 0))],
        out_specs=pl.BlockSpec((1, part, LANES), lambda e: (e, 0, 0)),
        out_shape=jax.ShapeDtypeStruct((devices, part, LANES), jnp.float32),
        cost_estimate=pl.CostEstimate(
            flops=6 * devices * part * rows * wide, bytes_accessed=8 * devices * rows * wide, transcendentals=0
        ),
        name="row_stage",
    )(high, low, table)


def lane_kernel(block, x_ref, mc_ref, ms_ref, jc_ref, js_ref, table_ref, *refs):
    re_ref, im_ref, prob_ref = refs[-3:]
    count = x_ref.shape[0]
    reals, imags = fourier([x_ref[j, 0] for j in range(count)], [x_ref[j, 1] for j in range(count)])
    mc, ms = mc_ref[...], ms_ref[...]
    highs, lows = [], []
    for j in range(count):
        jc, js = jc_ref[j : j + 1, :], js_ref[j : j + 1, :]
        c = mc * jc - ms * js
        s = mc * js + ms * jc
        rh, rl = halves(reals[j] * c - imags[j] * s)
        ih, il = halves(reals[j] * s + imags[j] * c)
        highs.append(jnp.concatenate([rh, ih], axis=1))
        lows.append(jnp.concatenate([rl, il], axis=1))
    high, low = jnp.concatenate(highs, axis=0), jnp.concatenate(lows, axis=0)
    dot = functools.partial(jnp.dot, preferred_element_type=jnp.float32)
    mixed = dot(high, table_ref[0]) + dot(high, table_ref[1]) + dot(low, table_ref[0])
    cube = jnp.swapaxes(mixed.reshape(count, block, 2 * LANES), 0, 1)
    re, im = cube[:, :, :LANES], cube[:, :, LANES:]
    re_ref[...] = re
    im_ref[...] = im
    prob_ref[...] = re * re + im * im


def lane_stage(x, previous, index, rows, mid, inner, table):
    count, _, part, lanes = x.shape
    block = 16
    first = index * (part // block)
    mspec = pl.BlockSpec((block, lanes), lambda i: (first + i, 0))
    jspec = pl.BlockSpec((count, lanes), lambda i: (0, 0))
    out = pl.BlockSpec((block, count, lanes), lambda i: (first + i, 0, 0))
    shape = jax.ShapeDtypeStruct((rows, count, lanes), jnp.float32)
    arguments = [x, *mid, *inner, table]
    specs = [
        pl.BlockSpec((count, 2, block, lanes), lambda i: (0, 0, i, 0)),
        mspec, mspec, jspec, jspec,
        pl.BlockSpec((2, 2 * lanes, 2 * lanes), lambda i: (0, 0, 0)),
    ]
    aliases = {}
    if previous is not None:
        aliases = {len(arguments) + k: k for k in range(3)}
        arguments += previous
        specs += [pl.BlockSpec(memory_space=pl.ANY)] * 3
    return pl.pallas_call(
        functools.partial(lane_kernel, block),
        grid=(part // block,),
        in_specs=specs,
        out_specs=[out, out, out],
        out_shape=[shape, shape, shape],
        input_output_aliases=aliases,
        cost_estimate=pl.CostEstimate(
            flops=20 * count * part * lanes * lanes, bytes_accessed=20 * count * part * lanes, transcendentals=0
        ),
        name="lane_stage",
    )(*arguments)


def exchange(x):
    return lax.all_to_all(x, AXES, split_axis=0, concat_axis=0, tiled=True)


def on_device(state_re, state_im):
    devices = lax.axis_size(AXES)
    local = state_re.shape[0]
    total = devices * local
    rows = local // (devices * LANES)
    me = lax.axis_index(AXES).astype(jnp.int32)
    rev_d, rev_a, rev_l = reversed_bits(devices), reversed_bits(rows), reversed_bits(LANES)

    def outgoing(values):
        return jnp.swapaxes(values.reshape(rows, devices, LANES), 0, 1)

    got_re, got_im = exchange(outgoing(state_re)), exchange(outgoing(state_im))

    a_index = jnp.arange(rows, dtype=jnp.int32)
    turn = phases((a_index[:, None] * (devices * LANES) + me * LANES) * rev_d[None, :], total)
    high, low = device_stage(got_re, got_im, *turn)

    def row_table(part):
        c, s = phases(part[:, None] * (a_index[None, :] * devices + me), rows * devices)
        return jnp.stack(table_halves(jnp.concatenate([c, s], axis=0)))

    k_here = jnp.sum(jnp.where(jnp.arange(devices) == me, rev_d, 0))
    lane = np.arange(LANES, dtype=np.int32)
    mid = phases((k_here + devices * rev_a)[:, None] * lane[None, :], total)
    angle = (rev_d[:, None] * lane[None, :] % (devices * LANES)) * (2.0 * math.pi / (devices * LANES))
    inner = (jnp.asarray(np.cos(angle), jnp.float32), jnp.asarray(np.sin(angle), jnp.float32))
    angle = (lane[:, None] * rev_l[None, :] % LANES) * (2.0 * math.pi / LANES)
    c, s = np.cos(angle) / math.sqrt(total), np.sin(angle) / math.sqrt(total)
    table = jnp.stack(table_halves(jnp.asarray(np.block([[c, s], [-s, c]]), jnp.float32)))

    part = rows // CHUNKS
    arrived = []
    for index in range(CHUNKS):
        sent = row_stage(high, low, row_table(rev_a[index * part : (index + 1) * part]))
        arrived.append(exchange(sent))
    outs = None
    for index in range(CHUNKS):
        x = arrived[index].reshape(devices, 2, part, LANES)
        outs = lane_stage(x, outs, index, rows, mid, inner, table)
    return tuple(values.reshape(local) for values in outs)


def solution(mesh):
    spec = P(AXES)
    return jax.shard_map(
        on_device, mesh=mesh, in_specs=(spec, spec), out_specs=(spec, spec, spec), check_vma=False
    )
```

```python
import functools
import math

import jax
import jax.numpy as jnp
import numpy as np
from jax import lax
from jax.experimental import pallas as pl
from jax.experimental.pallas import tpu as pltpu
from jax.sharding import PartitionSpec as P

AXES = ("gx", "gy", "gz")
LANES = 128
SLICES = 2


def reversed_bits(count):
    bits = count.bit_length() - 1
    values = np.arange(count)
    result = np.zeros(count, np.int32)
    for place in range(bits):
        result += ((values >> place) & 1) << (bits - 1 - place)
    return result.astype(np.int32)


def phases(product, modulus):
    angle = (product % modulus).astype(jnp.float32) * (2.0 * math.pi / modulus)
    return jnp.cos(angle), jnp.sin(angle)


def halves(values):
    high = values.astype(jnp.bfloat16)
    low = (values - high.astype(jnp.float32)).astype(jnp.bfloat16)
    return high, low


def table_halves(values):
    high = lax.reduce_precision(values, 8, 7)
    return high.astype(jnp.bfloat16), (values - high).astype(jnp.bfloat16)


def fourier(reals, imags):
    count = len(reals)
    span = count // 2
    reals, imags = list(reals), list(imags)
    while span >= 1:
        for start in range(0, count, 2 * span):
            for offset in range(span):
                top, bottom = start + offset, start + offset + span
                ar, ai, br, bi = reals[top], imags[top], reals[bottom], imags[bottom]
                reals[top], imags[top] = ar + br, ai + bi
                dr, di = ar - br, ai - bi
                if offset == 0:
                    reals[bottom], imags[bottom] = dr, di
                elif 2 * offset == span:
                    reals[bottom], imags[bottom] = -di, dr
                else:
                    angle = math.pi * offset / span
                    c, s = math.cos(angle), math.sin(angle)
                    if 4 * offset == span:
                        reals[bottom], imags[bottom] = (dr - di) * c, (dr + di) * c
                    elif 4 * offset == 3 * span:
                        reals[bottom], imags[bottom] = -(dr + di) * s, (dr - di) * s
                    else:
                        reals[bottom], imags[bottom] = dr * c - di * s, dr * s + di * c
        span //= 2
    return reals, imags


def gather(source, scratch, me):
    if len(source) == 1:
        return lambda d: (source[0][d, 0], source[0][d, 1])
    for slot, ref in enumerate(source):
        scratch[jnp.bitwise_xor(me, slot)] = ref[...]
    return lambda d: (scratch[d, 0], scratch[d, 1])


def block_specs(source, block, offset):
    if len(source) == 1:
        devices = source[0].shape[0]
        return [pl.BlockSpec((devices, 2, block, LANES), lambda i: (0, 0, offset + i, 0))]
    return [pl.BlockSpec((2, block, LANES), lambda i: (0, offset + i, 0)) for _ in source]


def scratches(source, block):
    return [pltpu.VMEM((len(source), 2, block, LANES), jnp.float32)] if len(source) > 1 else []


SCALAR = pl.BlockSpec(memory_space=pltpu.SMEM)
ANYWHERE = pl.BlockSpec(memory_space=pl.ANY)


def pack_kernel(many, me_ref, re_ref, im_ref, after_ref, *refs):
    for side, ref in enumerate((re_ref, im_ref)):
        turned = jnp.swapaxes(ref[:, 0], 0, 1)
        if not many:
            refs[0][:, side] = turned
            continue
        refs[-1][:, side] = turned
    if many:
        for slot, ref in enumerate(refs[:-1]):
            ref[...] = refs[-1][jnp.bitwise_xor(me_ref[0], slot)]


def pack_stage(me, re, im, c, many, after):
    rows, _, devices, lanes = re.shape
    block = min(16, rows)
    spec = pl.BlockSpec((block, 1, devices, lanes), lambda i: (i, c, 0, 0))
    if many:
        outs = [pl.BlockSpec((2, block, lanes), lambda i: (0, i, 0))] * devices
        shapes = [jax.ShapeDtypeStruct((2, rows, lanes), jnp.float32)] * devices
        scratch = [pltpu.VMEM((devices, 2, block, lanes), jnp.float32)]
    else:
        outs = [pl.BlockSpec((devices, 2, block, lanes), lambda i: (0, 0, i, 0))]
        shapes = [jax.ShapeDtypeStruct((devices, 2, rows, lanes), jnp.float32)]
        scratch = []
    return pl.pallas_call(
        functools.partial(pack_kernel, many),
        grid=(rows // block,),
        in_specs=[SCALAR, spec, spec, ANYWHERE],
        out_specs=outs,
        out_shape=shapes,
        scratch_shapes=scratch,
        cost_estimate=pl.CostEstimate(
            flops=40 * devices * rows * lanes, bytes_accessed=16 * devices * rows * lanes, transcendentals=0
        ),
        name="pack_stage",
    )(me, re, im, after)


def device_kernel(sources, me_ref, after_ref, cos_ref, sin_ref, *refs):
    high_ref, low_ref = refs[sources : sources + 2]
    me = me_ref[0]
    block_of = gather(refs[:sources], refs[-1], me)
    count = cos_ref.shape[1]
    blocks = [block_of(d) for d in range(count)]
    reals, imags = fourier([b[0] for b in blocks], [b[1] for b in blocks])
    for e in range(count):
        c, s = cos_ref[:, e : e + 1], sin_ref[:, e : e + 1]
        slot = jnp.bitwise_xor(me, e)
        for side, part in enumerate((reals[e] * c - imags[e] * s, reals[e] * s + imags[e] * c)):
            high_ref[slot, side], low_ref[slot, side] = halves(part)


def device_stage(me, source, turn, after):
    rows, devices = turn[0].shape
    block = 16
    table = pl.BlockSpec((block, devices), lambda i: (i, 0))
    out = pl.BlockSpec((devices, 2, block, LANES), lambda i: (0, 0, i, 0))
    shape = jax.ShapeDtypeStruct((devices, 2, rows, LANES), jnp.bfloat16)
    return pl.pallas_call(
        functools.partial(device_kernel, len(source)),
        grid=(rows // block,),
        in_specs=[SCALAR, ANYWHERE, table, table, *block_specs(source, block, 0)],
        out_specs=[out, out],
        out_shape=[shape, shape],
        scratch_shapes=scratches(source, block),
        cost_estimate=pl.CostEstimate(
            flops=200 * devices * rows * LANES, bytes_accessed=16 * devices * rows * LANES, transcendentals=0
        ),
        name="device_stage",
    )(me, after, *turn, *source)


def row_kernel(many, me_ref, high_ref, low_ref, table_ref, *refs):
    devices = high_ref.shape[0]
    dot = functools.partial(jnp.dot, preferred_element_type=jnp.float32)
    for slot in range(0, devices, 2):
        high = jnp.concatenate([high_ref[slot], high_ref[slot + 1]], axis=1)
        low = jnp.concatenate([low_ref[slot], low_ref[slot + 1]], axis=1)
        mixed = dot(table_ref[0], high) + dot(table_ref[1], high) + dot(table_ref[0], low)
        start, first = 0, 0
        for listed in many:
            for e in range(2):
                lanes = slice(LANES * e, LANES * (e + 1))
                if listed:
                    ref = refs[first + slot + e]
                    ref[...] = mixed[start : start + ref.shape[0], lanes]
                else:
                    ref = refs[first]
                    ref[jnp.bitwise_xor(me_ref[0], slot + e)] = mixed[start : start + ref.shape[1], lanes]
            start += ref.shape[-2]
            first += devices if listed else 1


def row_stage(me, high, low, table, parts, many):
    devices, _, rows, _ = high.shape
    shapes = []
    for part, listed in zip(parts, many):
        one = (2 * part, LANES)
        shapes += [jax.ShapeDtypeStruct(one if listed else (devices, *one), jnp.float32)] * (devices if listed else 1)
    whole = pl.BlockSpec(memory_space=pltpu.VMEM)
    outs = pl.pallas_call(
        functools.partial(row_kernel, many),
        in_specs=[SCALAR, whole, whole, whole],
        out_specs=[whole] * len(shapes),
        out_shape=shapes,
        cost_estimate=pl.CostEstimate(
            flops=24 * devices * rows * rows * LANES, bytes_accessed=16 * devices * rows * LANES, transcendentals=0
        ),
        name="row_stage",
    )(me, high.reshape(devices, 2 * rows, LANES), low.reshape(devices, 2 * rows, LANES), table)
    results = []
    for part, listed in zip(parts, many):
        taken = devices if listed else 1
        shape = (2, part, LANES) if listed else (devices, 2, part, LANES)
        results.append([y.reshape(shape) for y in outs[:taken]])
        outs = outs[taken:]
    return results


def lane_kernel(block, counts, me_ref, mc_ref, ms_ref, jc_ref, js_ref, table_ref, *refs):
    me = me_ref[0]
    scratch = list(refs[len(refs) - sum(n > 1 for n in counts) :])
    re_ref, im_ref, prob_ref = refs[len(refs) - len(scratch) - 3 : len(refs) - len(scratch)]
    count = jc_ref.shape[0]
    blocks = []
    for n in counts:
        block_of = gather(refs[:n], scratch.pop(0) if n > 1 else None, me)
        refs = refs[n:]
        blocks += [block_of(j) for j in range(count // len(counts))]
    reals, imags = fourier([b[0] for b in blocks], [b[1] for b in blocks])
    mc, ms = mc_ref[...], ms_ref[...]
    highs, lows = [], []
    for j in range(count):
        jc, js = jc_ref[j : j + 1, :], js_ref[j : j + 1, :]
        c = mc * jc - ms * js
        s = mc * js + ms * jc
        rh, rl = halves(reals[j] * c - imags[j] * s)
        ih, il = halves(reals[j] * s + imags[j] * c)
        highs.append(jnp.concatenate([rh, ih], axis=1))
        lows.append(jnp.concatenate([rl, il], axis=1))
    high, low = jnp.concatenate(highs, axis=0), jnp.concatenate(lows, axis=0)
    dot = functools.partial(jnp.dot, preferred_element_type=jnp.float32)
    mixed = dot(high, table_ref[0]) + dot(high, table_ref[1]) + dot(low, table_ref[0])
    cube = jnp.swapaxes(mixed.reshape(count, block, 2 * LANES), 0, 1)
    re, im = cube[:, :, :LANES], cube[:, :, LANES:]
    re_ref[...] = re
    im_ref[...] = im
    prob_ref[...] = re * re + im * im


def lane_stage(me, sources, previous, start, part, rows, mid, inner, table):
    count = inner[0].shape[0]
    block = 16 if part % 16 == 0 and start % 16 == 0 else 8
    first = start // block
    mspec = pl.BlockSpec((block, LANES), lambda i: (first + i, 0))
    jspec = pl.BlockSpec((count, LANES), lambda i: (0, 0))
    out = pl.BlockSpec((block, count, LANES), lambda i: (first + i, 0, 0))
    shape = jax.ShapeDtypeStruct((rows, count, LANES), jnp.float32)
    arguments = [me, *mid, *inner, table]
    specs = [SCALAR, mspec, mspec, jspec, jspec, pl.BlockSpec((2, 2 * LANES, 2 * LANES), lambda i: (0, 0, 0))]
    scratch = []
    for source, base in sources:
        arguments += source
        specs += block_specs(source, block, (start - base) // block)
        scratch += scratches(source, block)
    aliases = {}
    if previous is not None:
        aliases = {len(arguments) + k: k for k in range(3)}
        arguments += previous
        specs += [ANYWHERE] * 3
    return pl.pallas_call(
        functools.partial(lane_kernel, block, tuple(len(source) for source, _ in sources)),
        grid=(part // block,),
        in_specs=specs,
        out_specs=[out, out, out],
        out_shape=[shape, shape, shape],
        scratch_shapes=scratch,
        input_output_aliases=aliases,
        cost_estimate=pl.CostEstimate(
            flops=20 * count * part * LANES * LANES, bytes_accessed=20 * count * part * LANES, transcendentals=0
        ),
        name="lane_stage",
    )(*arguments)


def exchange(source):
    if len(source) > 1:
        count = len(source)
        return [source[0]] + [
            lax.ppermute(source[s], AXES, [(i, i ^ s) for i in range(count)]) for s in range(1, count)
        ]
    devices, _, rows, lanes = source[0].shape
    flat = source[0].reshape(devices, 2 * rows, lanes)
    got = lax.all_to_all(flat, AXES, split_axis=0, concat_axis=0, tiled=True)
    return [got.reshape(devices, 2, rows, lanes)]


def on_device(state_re, state_im):
    devices = lax.axis_size(AXES)
    local = state_re.shape[0]
    total = devices * local
    rows = local // (devices * SLICES * LANES)
    me = lax.axis_index(AXES).astype(jnp.int32)
    here = me.reshape(1)
    rev_d, rev_a, rev_l = reversed_bits(devices), reversed_bits(rows), reversed_bits(LANES)
    a_index = jnp.arange(rows, dtype=jnp.int32)
    inside = devices * SLICES
    shape = (rows, SLICES, devices, LANES)
    parts = (3 * rows // 4, rows // 4)

    def middle(source, c, parts, many, after):
        turn = phases((a_index[:, None] * (inside * LANES) + (c * devices + me) * LANES) * rev_d[None, :], total)
        high, low = device_stage(here, source, turn, after)
        cosine, sine = phases(rev_a[:, None] * (a_index[None, :] * inside + c * devices + me), rows * inside)
        pieces, start = [], 0
        for part in parts:
            cos_p, sin_p = cosine[start : start + part], sine[start : start + part]
            pieces += [jnp.concatenate([cos_p, -sin_p], axis=1), jnp.concatenate([sin_p, cos_p], axis=1)]
            start += part
        table = jnp.stack(table_halves(jnp.concatenate(pieces, axis=0)))
        return row_stage(here, high, low, table, parts, many)

    k_here = jnp.sum(jnp.where(jnp.arange(devices) == me, rev_d, 0))
    lane = np.arange(LANES, dtype=np.int32)
    mid = phases((k_here + devices * rev_a)[:, None] * lane[None, :], total)
    angle = (reversed_bits(inside)[:, None] * lane[None, :] % (inside * LANES)) * (2.0 * math.pi / (inside * LANES))
    inner = (jnp.asarray(np.cos(angle), jnp.float32), jnp.asarray(np.sin(angle), jnp.float32))
    angle = (lane[:, None] * rev_l[None, :] % LANES) * (2.0 * math.pi / LANES)
    c, s = np.cos(angle) / math.sqrt(total), np.sin(angle) / math.sqrt(total)
    table = jnp.stack(table_halves(jnp.asarray(np.block([[c, s], [-s, c]]), jnp.float32)))

    re, im = state_re.reshape(shape), state_im.reshape(shape)
    packed = pack_stage(here, re, im, 0, True, here)
    first = exchange(packed)
    second = exchange(pack_stage(here, re, im, 1, False, packed[0]))
    (sent,) = middle(first, 0, (rows,), (True,), here)
    early = exchange(sent)
    late = [exchange(piece) for piece in middle(second, 1, parts, (False, True), sent[0])]
    outs, start = None, 0
    for piece, part in zip(late, parts):
        sources = [(early, 0), (piece, start)]
        outs = lane_stage(here, sources, outs, start, part, rows, mid, inner, table)
        start += part
    return tuple(values.reshape(local) for values in outs)


def solution(mesh):
    spec = P(AXES)
    return jax.shard_map(
        on_device, mesh=mesh, in_specs=(spec, spec), out_specs=(spec, spec, spec), check_vma=False
    )
```

```python
import functools
import math

import jax
import jax.numpy as jnp
import numpy as np
from jax import lax
from jax.experimental import pallas as pl
from jax.experimental.pallas import tpu as pltpu
from jax.sharding import PartitionSpec as P


AXES = ("gx", "gy", "gz")
LANES = 128
SLICES = 4
SWAP = 4
TILE = 128
GROUPS = ((2, 3), (1, 0))

SCALAR = pl.BlockSpec(memory_space=pltpu.SMEM)
ANYWHERE = pl.BlockSpec(memory_space=pl.ANY)
WHOLE = pl.BlockSpec(memory_space=pltpu.VMEM)


def reversed_bits(count):
    bits = count.bit_length() - 1
    values = np.arange(count)
    result = np.zeros(count, np.int32)
    for place in range(bits):
        result += ((values >> place) & 1) << (bits - 1 - place)
    return result.astype(np.int32)


def phases(product, modulus):
    angle = (product % modulus).astype(jnp.float32) * (2.0 * math.pi / modulus)
    return jnp.cos(angle), jnp.sin(angle)


def halves(values):
    high = values.astype(jnp.bfloat16)
    low = (values - high.astype(jnp.float32)).astype(jnp.bfloat16)
    return high, low


def table_halves(values):
    high = lax.reduce_precision(values, 8, 7)
    return high.astype(jnp.bfloat16), (values - high).astype(jnp.bfloat16)


def fourier(reals, imags):
    count = len(reals)
    span = count // 2
    reals, imags = list(reals), list(imags)
    while span >= 1:
        for start in range(0, count, 2 * span):
            for offset in range(span):
                top, bottom = start + offset, start + offset + span
                ar, ai, br, bi = reals[top], imags[top], reals[bottom], imags[bottom]
                reals[top], imags[top] = ar + br, ai + bi
                dr, di = ar - br, ai - bi
                if offset == 0:
                    reals[bottom], imags[bottom] = dr, di
                elif 2 * offset == span:
                    reals[bottom], imags[bottom] = -di, dr
                else:
                    angle = math.pi * offset / span
                    c, s = math.cos(angle), math.sin(angle)
                    if 4 * offset == span:
                        reals[bottom], imags[bottom] = (dr - di) * c, (dr + di) * c
                    elif 4 * offset == 3 * span:
                        reals[bottom], imags[bottom] = -(dr + di) * s, (dr - di) * s
                    else:
                        reals[bottom], imags[bottom] = dr * c - di * s, dr * s + di * c
        span //= 2
    return reals, imags


def pack_kernel(first, z_ref, re_ref, im_ref, *refs):
    outs = refs[-SWAP:]
    block, tile, lanes = re_ref.shape
    for side, ref in enumerate((re_ref, im_ref)):
        flat = ref.reshape(block * tile, lanes)
        for slot, out_ref in enumerate(outs):
            place = first + jnp.bitwise_xor(z_ref[0], slot)
            out_ref[side] = flat[pl.ds(place, block, stride=tile), :]


def pack_stage(z, re, im, c, after):
    rows, _, lanes = re.shape
    block, tile = 128, 8
    spec = pl.BlockSpec((block, tile, lanes), lambda i: (i, c * SWAP // tile, 0))
    out = pl.BlockSpec((2, block, lanes), lambda i: (0, i, 0))
    return pl.pallas_call(
        functools.partial(pack_kernel, c * SWAP % tile),
        grid=(rows // block,),
        in_specs=[SCALAR, spec, spec] + [ANYWHERE] * len(after),
        out_specs=[out] * SWAP,
        out_shape=[jax.ShapeDtypeStruct((2, rows, lanes), jnp.float32)] * SWAP,
        cost_estimate=pl.CostEstimate(flops=40 << 20, bytes_accessed=8 << 20, transcendentals=0),
        name="pack_stage",
    )(z, re, im, *after)


def butterfly(mine, theirs, sign, cosine, sine):
    r, i = theirs[0] + sign * mine[0], theirs[1] + sign * mine[1]
    return r * cosine - i * sine, r * sine + i * cosine


def per_slot(refs):
    return [refs[0].at[s] for s in range(SWAP)] if len(refs) == 1 else refs


def slot_spec(listed, block):
    if listed:
        return [pl.BlockSpec((2, block, LANES), lambda i: (0, i, 0))] * SWAP
    return [pl.BlockSpec((SWAP, 2, block, LANES), lambda i: (0, 0, i, 0))]


def slot_shape(listed, rows):
    shape = (2, rows, LANES) if listed else (SWAP, 2, rows, LANES)
    return [jax.ShapeDtypeStruct(shape, jnp.float32)] * (SWAP if listed else 1)


def mix_kernel(inputs, coef_ref, after_ref, *refs):
    mine, theirs, outs = (
        per_slot(part) for part in (refs[:inputs], refs[inputs : 2 * inputs], refs[2 * inputs :])
    )
    for s in range(SWAP):
        r, i = butterfly(mine[s], theirs[s], coef_ref[2 * SWAP], coef_ref[s], coef_ref[SWAP + s])
        outs[s][0], outs[s][1] = r, i


def mix_stage(coef, mine, theirs, listed, after):
    rows = mine[0].shape[-2]
    block = 128
    return pl.pallas_call(
        functools.partial(mix_kernel, len(mine)),
        grid=(rows // block,),
        in_specs=[SCALAR, ANYWHERE] + slot_spec(len(mine) > 1, block) * 2,
        out_specs=slot_spec(listed, block),
        out_shape=slot_shape(listed, rows),
        cost_estimate=pl.CostEstimate(flops=20 << 20, bytes_accessed=6 << 20, transcendentals=0),
        name="mix_stage",
    )(coef, after, *mine, *theirs)


def swap_kernel(z_ref, coef_ref, turn_ref, after_ref, mine_ref, theirs_ref, *refs):
    outs, scratch = per_slot(refs[:-1]), refs[-1]
    reals, imags = [], []
    for place in range(SWAP):
        slot = jnp.bitwise_xor(z_ref[0], place)
        r, i = butterfly(
            mine_ref.at[slot], theirs_ref.at[slot], coef_ref[2 * SWAP], coef_ref[place], coef_ref[SWAP + place]
        )
        reals.append(r)
        imags.append(i)
    reals, imags = fourier(reals, imags)
    for place in range(SWAP):
        c, s = turn_ref[place], turn_ref[SWAP + place]
        scratch[place, 0] = reals[place] * c - imags[place] * s
        scratch[place, 1] = reals[place] * s + imags[place] * c
    for slot in range(SWAP):
        outs[slot][...] = scratch[jnp.bitwise_xor(z_ref[0], slot)]


def swap_stage(z, coef, turn, mine, theirs, listed, after):
    rows = mine.shape[-2]
    block = 128
    full = slot_spec(False, block)
    return pl.pallas_call(
        swap_kernel,
        grid=(rows // block,),
        in_specs=[SCALAR, SCALAR, SCALAR, ANYWHERE] + full * 2,
        out_specs=slot_spec(listed, block),
        out_shape=slot_shape(listed, rows),
        scratch_shapes=[pltpu.VMEM((SWAP, 2, block, LANES), jnp.float32)],
        cost_estimate=pl.CostEstimate(flops=30 << 20, bytes_accessed=6 << 20, transcendentals=0),
        name="swap_stage",
    )(z, coef, turn, after, mine, theirs)


def row_kernel(c, slots, sizes, coef_ref, after_ref, tc_ref, ts_ref, rc_ref, rs_ref, table_ref, *refs):
    refs, (high_ref, low_ref) = refs[:-2], refs[-2:]
    inputs = len(slots) if len(slots) < SWAP else 1
    mine, theirs, outs = refs[:inputs], refs[inputs : 2 * inputs], refs[2 * inputs :]
    if len(slots) == SWAP:
        mine, theirs = per_slot(mine), per_slot(theirs)
    dot = functools.partial(jnp.dot, preferred_element_type=jnp.float32)
    for n, s in enumerate(slots):
        r, i = butterfly(mine[n], theirs[n], coef_ref[2 * SWAP], coef_ref[0], coef_ref[SWAP])
        cosine, sine = tc_ref[:, s : s + 1], ts_ref[:, s : s + 1]
        high_ref[:, :LANES], low_ref[:, :LANES] = halves(r * cosine - i * sine)
        high_ref[:, LANES:], low_ref[:, LANES:] = halves(r * sine + i * cosine)
        base = 0
        for part, size in enumerate(sizes):
            out_ref = outs[part * len(slots) + n]

            def tile(m, carry, out_ref=out_ref, base=base):
                high = high_ref[...]
                mixed = dot(table_ref[base + m, 0], high) + dot(table_ref[base + m, 1], high)
                mixed += dot(table_ref[base + m, 0], low_ref[...])
                yr = mixed[:TILE, :LANES] - mixed[TILE:, LANES:]
                yi = mixed[TILE:, :LANES] + mixed[:TILE, LANES:]
                here = pl.ds(pl.multiple_of((base + m) * TILE, TILE), TILE)
                cosine, sine = rc_ref[here, c : c + 1], rs_ref[here, c : c + 1]
                there = pl.ds(pl.multiple_of(m * TILE, TILE), TILE)
                out_ref[0, there, :] = yr * cosine - yi * sine
                out_ref[1, there, :] = yr * sine + yi * cosine
                return carry

            lax.fori_loop(0, size // TILE, tile, 0)
            base += size // TILE


def row_stage(coef, turn, scale, table, mine, theirs, c, slots, sizes, after):
    rows = mine[0].shape[-2]
    shapes = [jax.ShapeDtypeStruct((2, size, LANES), jnp.float32) for size in sizes for _ in slots]
    outs = pl.pallas_call(
        functools.partial(row_kernel, c, slots, sizes),
        in_specs=[SCALAR, ANYWHERE] + [WHOLE] * (5 + 2 * len(mine)),
        out_specs=[WHOLE] * len(shapes),
        out_shape=shapes,
        scratch_shapes=[pltpu.VMEM((rows, 2 * LANES), jnp.bfloat16)] * 2,
        cost_estimate=pl.CostEstimate(flops=len(slots) * (100 << 20), bytes_accessed=8 << 20, transcendentals=0),
        name="row_stage",
    )(coef, after, *turn, *scale, table, *mine, *theirs)
    return [outs[k * len(slots) : (k + 1) * len(slots)] for k in range(len(sizes))]


def lane_kernel(block, z_ref, mc_ref, ms_ref, jc_ref, js_ref, table_ref, *refs):
    count = jc_ref.shape[0]
    scratch = refs[-1]
    re_ref, im_ref, prob_ref = refs[-4:-1]
    for n in range(count):
        scratch[(n // SWAP) * SWAP + jnp.bitwise_xor(z_ref[0], n % SWAP)] = refs[n][...]
    reals, imags = fourier([scratch[n, 0] for n in range(count)], [scratch[n, 1] for n in range(count)])
    mc, ms = mc_ref[...], ms_ref[...]
    highs, lows = [], []
    for j in range(count):
        jc, js = jc_ref[j : j + 1, :], js_ref[j : j + 1, :]
        c = mc * jc - ms * js
        s = mc * js + ms * jc
        rh, rl = halves(reals[j] * c - imags[j] * s)
        ih, il = halves(reals[j] * s + imags[j] * c)
        highs.append(jnp.concatenate([rh, ih], axis=1))
        lows.append(jnp.concatenate([rl, il], axis=1))
    high, low = jnp.concatenate(highs, axis=0), jnp.concatenate(lows, axis=0)
    dot = functools.partial(jnp.dot, preferred_element_type=jnp.float32)
    mixed = dot(high, table_ref[0]) + dot(high, table_ref[1]) + dot(low, table_ref[0])
    cube = jnp.swapaxes(mixed.reshape(count, block, 2 * LANES), 0, 1)
    re, im = cube[:, :, :LANES], cube[:, :, LANES:]
    re_ref[...] = re
    im_ref[...] = im
    prob_ref[...] = re * re + im * im


def lane_stage(z, sources, previous, start, part, rows, mid, inner, table):
    count = inner[0].shape[0]
    block = 32
    first = start // block
    mspec = pl.BlockSpec((block, LANES), lambda i: (first + i, 0))
    jspec = pl.BlockSpec((count, LANES), lambda i: (0, 0))
    out = pl.BlockSpec((block, count, LANES), lambda i: (first + i, 0, 0))
    shape = jax.ShapeDtypeStruct((rows, count, LANES), jnp.float32)
    arguments = [z, *mid, *inner, table]
    specs = [SCALAR, mspec, mspec, jspec, jspec, pl.BlockSpec((2, 2 * LANES, 2 * LANES), lambda i: (0, 0, 0))]
    for source, base in sources:
        offset = (start - base) // block
        arguments += source
        specs += [pl.BlockSpec((2, block, LANES), lambda i, offset=offset: (0, offset + i, 0))] * SWAP
    aliases = {}
    kernel = functools.partial(lane_kernel, block)
    if previous is not None:
        aliases = {len(arguments) + k: k for k in range(3)}
        arguments += previous
        specs += [ANYWHERE] * 3
    return pl.pallas_call(
        kernel,
        grid=(part // block,),
        in_specs=specs,
        out_specs=[out, out, out],
        out_shape=[shape, shape, shape],
        scratch_shapes=[pltpu.VMEM((count, 2, block, LANES), jnp.float32)],
        input_output_aliases=aliases,
        cost_estimate=pl.CostEstimate(
            flops=20 * count * part * LANES * LANES, bytes_accessed=20 * count * part * LANES, transcendentals=0
        ),
        name="lane_stage",
    )(*arguments)


def on_device(state_re, state_im):
    devices = lax.axis_size(AXES)
    sizes = [lax.axis_size(axis) for axis in AXES]
    assert sizes[0] == 2 and sizes[1] == 2 and sizes[2] % SWAP == 0
    weights = sizes[2] // SWAP
    local = state_re.shape[0]
    total = devices * local
    inside = SLICES * SWAP
    rows = local // (inside * LANES)
    x, core, g = (lax.axis_index(axis).astype(jnp.int32) for axis in AXES)
    z, w = g // weights, g % weights
    zs = z.reshape(1)
    rev_a, rev_l, rev_z = reversed_bits(rows), reversed_bits(LANES), reversed_bits(SWAP)
    places = jnp.arange(SWAP, dtype=jnp.int32)
    slots = jnp.bitwise_xor(places, z)
    a_index = jnp.arange(rows, dtype=jnp.int32)
    w_bits = weights.bit_length() - 1
    rev_w = sum(((w >> t) & 1) << (w_bits - 1 - t) for t in range(w_bits))

    def flip(values, distance):
        return lax.ppermute(values, AXES, [(i, i ^ distance) for i in range(devices)])

    def coefficients(bit, exponents, modulus):
        c, s = phases(bit * exponents, modulus)
        sign = (1 - 2 * bit).astype(jnp.float32).reshape(1)
        return jnp.concatenate([c, s, sign])

    x_coef = coefficients(x, core * (devices // 4) + slots * weights + w, devices)
    core_coef = coefficients(core, places * weights + w, devices // 2)
    z_turn = jnp.concatenate(phases(rev_z * w, SWAP * weights))
    w_coef = {t: coefficients((w >> t) & 1, 0 * places + w % (1 << t), 2 << t) for t in range(w_bits)}
    low_k = x + 2 * core + 16 * rev_w
    k_slot = low_k + 4 * (2 * (slots & 1) + (slots >> 1))
    k_here = low_k + 4 * (2 * (z & 1) + (z >> 1))

    cosine, sine = phases(rev_a[:, None] * a_index[None, :], rows)
    tiles = (rows // TILE, TILE, rows)
    table = jnp.concatenate([cosine.reshape(tiles), sine.reshape(tiles)], axis=1)
    row_table = jnp.stack(table_halves(table), axis=1)
    offsets = jnp.arange(SLICES, dtype=jnp.int32) * SWAP + z
    scale = phases(rev_a[:, None] * offsets[None, :], rows * inside)
    turns = [
        phases((a_index[:, None] * (inside * LANES) + offsets[c] * LANES) * k_slot[None, :], total)
        for c in range(SLICES)
    ]

    lane = np.arange(LANES, dtype=np.int32)
    mid = phases((k_here + devices * rev_a)[:, None] * lane[None, :], total)
    angle = (reversed_bits(inside)[:, None] * lane[None, :] % (inside * LANES)) * (2.0 * math.pi / (inside * LANES))
    inner = (jnp.asarray(np.cos(angle), jnp.float32), jnp.asarray(np.sin(angle), jnp.float32))
    angle = (lane[:, None] * rev_l[None, :] % LANES) * (2.0 * math.pi / LANES)
    c, s = np.cos(angle) / math.sqrt(total), np.sin(angle) / math.sqrt(total)
    lane_table = jnp.stack(table_halves(jnp.asarray(np.block([[c, s], [-s, c]]), jnp.float32)))

    re, im = (v.reshape(rows, inside, LANES) for v in (state_re, state_im))
    chain = [zs]

    def kernel(function, *arguments):
        result = function(*arguments, chain[0])
        leaf = jax.tree.leaves(result)[0]
        chain[0] = leaf
        return result

    def swap_out(arrays):
        return [arrays[0]] + [flip(arrays[s], s * weights) for s in range(1, SWAP)]

    packed, inward, across, mixed, spread = {}, {}, {}, {}, {}
    parts = {k: (rows,) for k in range(SLICES)}
    parts[SLICES - 1] = (TILE,) * (rows // TILE)
    outward = {k: [[None] * SWAP for _ in sizes] for k, sizes in parts.items()}

    def pack(k, *after):
        packed[k] = pack_stage(zs, re, im, k, [chain[0], *after])
        chain[0] = packed[k][0]
        inward[k] = swap_out(packed[k])
        across[k] = [flip(packed[k][0], devices // 2)]

    def cross(k):
        across[k] += [flip(v, devices // 2) for v in inward[k][1:]]

    def mixing(k):
        (mixed[k],) = kernel(mix_stage, x_coef, inward[k], across[k], False)
        spread[k] = flip(mixed[k], devices // 4)

    def swapping(k):
        mixed[k] = kernel(swap_stage, zs, core_coef, z_turn, mixed[k], spread[k], True)
        for t in range(w_bits - 1, -1, -1):
            spread[k] = [None] * SWAP
            for s in sum(GROUPS, ()):
                spread[k][s] = flip(mixed[k][s], 1 << t)
            if t:
                mixed[k] = kernel(mix_stage, w_coef[t], mixed[k], spread[k], True)

    def finish(k, n):
        mine, theirs = ([v[k][s] for s in GROUPS[n]] for v in (mixed, spread))
        shared = (w_coef[0], turns[k], scale, row_table)
        pieces = kernel(row_stage, *shared, mine, theirs, k, GROUPS[n], parts[k])
        for p, piece in enumerate(pieces):
            for s, value in zip(GROUPS[n], piece):
                outward[k][p][s] = flip(value, s * weights) if s else value

    pack(0), pack(1, row_table, *scale, *turns[0]), pack(2), pack(3)
    cross(0), cross(1), mixing(0), swapping(0), mixing(1), cross(2)
    for k in range(1, SLICES):
        finish(k - 1, 0), swapping(k), finish(k - 1, 1)
        if k + 1 < SLICES:
            if k + 2 < SLICES:
                cross(k + 2)
            mixing(k + 1)
    finish(SLICES - 1, 0), finish(SLICES - 1, 1)
    outs, start, last = None, 0, SLICES - 1
    for n, part in enumerate(parts[last]):
        sources = [(outward[k][0], 0) for k in range(last)] + [(outward[last][n], start)]
        outs = lane_stage(zs, sources, outs, start, part, rows, mid, inner, lane_table)
        start += part
    return tuple(values.reshape(local) for values in outs)


def solution(mesh):
    spec = P(AXES)
    return jax.shard_map(
        on_device, mesh=mesh, in_specs=(spec, spec), out_specs=(spec, spec, spec), check_vma=False
    )
```

```python
import functools
import math

import jax
import jax.numpy as jnp
import numpy as np
from jax import lax
from jax.experimental import pallas as pl
from jax.experimental.pallas import tpu as pltpu
from jax.sharding import PartitionSpec as P


AXES = ("gx", "gy", "gz")
LANES = 128
SLICES = 4
SWAP = 4
TILE = 128
GROUPS = ((2, 3), (1, 0))

SCALAR = pl.BlockSpec(memory_space=pltpu.SMEM)
ANYWHERE = pl.BlockSpec(memory_space=pl.ANY)
WHOLE = pl.BlockSpec(memory_space=pltpu.VMEM)


def reversed_bits(count):
    bits = count.bit_length() - 1
    values = np.arange(count)
    result = np.zeros(count, np.int32)
    for place in range(bits):
        result += ((values >> place) & 1) << (bits - 1 - place)
    return result.astype(np.int32)


def phases(product, modulus):
    angle = (product % modulus).astype(jnp.float32) * (2.0 * math.pi / modulus)
    return jnp.cos(angle), jnp.sin(angle)


def halves(values):
    high = values.astype(jnp.bfloat16)
    low = (values - high.astype(jnp.float32)).astype(jnp.bfloat16)
    return high, low


def table_halves(values):
    high = lax.reduce_precision(values, 8, 7)
    return high.astype(jnp.bfloat16), (values - high).astype(jnp.bfloat16)


def fourier(reals, imags):
    count = len(reals)
    span = count // 2
    reals, imags = list(reals), list(imags)
    while span >= 1:
        for start in range(0, count, 2 * span):
            for offset in range(span):
                top, bottom = start + offset, start + offset + span
                ar, ai, br, bi = reals[top], imags[top], reals[bottom], imags[bottom]
                reals[top], imags[top] = ar + br, ai + bi
                dr, di = ar - br, ai - bi
                if offset == 0:
                    reals[bottom], imags[bottom] = dr, di
                elif 2 * offset == span:
                    reals[bottom], imags[bottom] = -di, dr
                else:
                    angle = math.pi * offset / span
                    c, s = math.cos(angle), math.sin(angle)
                    if 4 * offset == span:
                        reals[bottom], imags[bottom] = (dr - di) * c, (dr + di) * c
                    elif 4 * offset == 3 * span:
                        reals[bottom], imags[bottom] = -(dr + di) * s, (dr - di) * s
                    else:
                        reals[bottom], imags[bottom] = dr * c - di * s, dr * s + di * c
        span //= 2
    return reals, imags


def pack_kernel(first, z_ref, re_ref, im_ref, *refs):
    outs = refs[-SWAP:]
    block, tile, lanes = re_ref.shape
    for side, ref in enumerate((re_ref, im_ref)):
        flat = ref.reshape(block * tile, lanes)
        for slot, out_ref in enumerate(outs):
            place = first + jnp.bitwise_xor(z_ref[0], slot)
            out_ref[side] = flat[pl.ds(place, block, stride=tile), :]


def pack_stage(z, re, im, c, after):
    rows, _, lanes = re.shape
    block, tile = 256, 8
    spec = pl.BlockSpec((block, tile, lanes), lambda i: (i, c * SWAP // tile, 0))
    out = pl.BlockSpec((2, block, lanes), lambda i: (0, i, 0))
    return pl.pallas_call(
        functools.partial(pack_kernel, c * SWAP % tile),
        grid=(rows // block,),
        in_specs=[SCALAR, spec, spec] + [ANYWHERE] * len(after),
        out_specs=[out] * SWAP,
        out_shape=[jax.ShapeDtypeStruct((2, rows, lanes), jnp.float32)] * SWAP,
        cost_estimate=pl.CostEstimate(flops=40 << 20, bytes_accessed=8 << 20, transcendentals=0),
        name="pack_stage",
    )(z, re, im, *after)


def butterfly(mine, theirs, sign, cosine, sine):
    r, i = theirs[0] + sign * mine[0], theirs[1] + sign * mine[1]
    return r * cosine - i * sine, r * sine + i * cosine


def per_slot(refs):
    return [refs[0].at[s] for s in range(SWAP)] if len(refs) == 1 else refs


def slot_spec(listed, block):
    if listed:
        return [pl.BlockSpec((2, block, LANES), lambda i: (0, i, 0))] * SWAP
    return [pl.BlockSpec((SWAP, 2, block, LANES), lambda i: (0, 0, i, 0))]


def slot_shape(listed, rows):
    shape = (2, rows, LANES) if listed else (SWAP, 2, rows, LANES)
    return [jax.ShapeDtypeStruct(shape, jnp.float32)] * (SWAP if listed else 1)


def mix_kernel(inputs, coef_ref, after_ref, *refs):
    mine, theirs, outs = (
        per_slot(part) for part in (refs[:inputs], refs[inputs : 2 * inputs], refs[2 * inputs :])
    )
    for s in range(SWAP):
        r, i = butterfly(mine[s], theirs[s], coef_ref[2 * SWAP], coef_ref[s], coef_ref[SWAP + s])
        outs[s][0], outs[s][1] = r, i


def mix_stage(coef, mine, theirs, listed, after):
    rows = mine[0].shape[-2]
    block = 128
    return pl.pallas_call(
        functools.partial(mix_kernel, len(mine)),
        grid=(rows // block,),
        in_specs=[SCALAR, ANYWHERE] + slot_spec(len(mine) > 1, block) * 2,
        out_specs=slot_spec(listed, block),
        out_shape=slot_shape(listed, rows),
        cost_estimate=pl.CostEstimate(flops=20 << 20, bytes_accessed=6 << 20, transcendentals=0),
        name="mix_stage",
    )(coef, after, *mine, *theirs)


def swap_kernel(z_ref, coef_ref, turn_ref, after_ref, mine_ref, theirs_ref, *refs):
    outs, scratch = per_slot(refs[:-1]), refs[-1]
    reals, imags = [], []
    for place in range(SWAP):
        slot = jnp.bitwise_xor(z_ref[0], place)
        r, i = butterfly(
            mine_ref.at[slot], theirs_ref.at[slot], coef_ref[2 * SWAP], coef_ref[place], coef_ref[SWAP + place]
        )
        reals.append(r)
        imags.append(i)
    reals, imags = fourier(reals, imags)
    for place in range(SWAP):
        c, s = turn_ref[place], turn_ref[SWAP + place]
        scratch[place, 0] = reals[place] * c - imags[place] * s
        scratch[place, 1] = reals[place] * s + imags[place] * c
    for slot in range(SWAP):
        outs[slot][...] = scratch[jnp.bitwise_xor(z_ref[0], slot)]


def swap_stage(z, coef, turn, mine, theirs, listed, after):
    rows = mine.shape[-2]
    block = 128
    full = slot_spec(False, block)
    return pl.pallas_call(
        swap_kernel,
        grid=(rows // block,),
        in_specs=[SCALAR, SCALAR, SCALAR, ANYWHERE] + full * 2,
        out_specs=slot_spec(listed, block),
        out_shape=slot_shape(listed, rows),
        scratch_shapes=[pltpu.VMEM((SWAP, 2, block, LANES), jnp.float32)],
        cost_estimate=pl.CostEstimate(flops=30 << 20, bytes_accessed=6 << 20, transcendentals=0),
        name="swap_stage",
    )(z, coef, turn, after, mine, theirs)


def row_kernel(slots, sizes, coef_ref, after_ref, tc_ref, ts_ref, rc_ref, rs_ref, table_ref, *refs):
    refs, (high_ref, low_ref) = refs[:-2], refs[-2:]
    inputs = len(slots) if len(slots) < SWAP else 1
    mine, theirs, outs = refs[:inputs], refs[inputs : 2 * inputs], refs[2 * inputs :]
    if len(slots) == SWAP:
        mine, theirs = per_slot(mine), per_slot(theirs)
    dot = functools.partial(jnp.dot, preferred_element_type=jnp.float32)
    for n, s in enumerate(slots):
        r, i = butterfly(mine[n], theirs[n], coef_ref[2 * SWAP], coef_ref[0], coef_ref[SWAP])
        cosine, sine = tc_ref[:, s : s + 1], ts_ref[:, s : s + 1]
        high_ref[:, :LANES], low_ref[:, :LANES] = halves(r * cosine - i * sine)
        high_ref[:, LANES:], low_ref[:, LANES:] = halves(r * sine + i * cosine)
        base = 0
        for part, size in enumerate(sizes):
            out_ref = outs[part * len(slots) + n]

            def tile(m, carry, out_ref=out_ref, base=base):
                high = high_ref[...]
                mixed = dot(table_ref[base + m, 0], high) + dot(table_ref[base + m, 1], high)
                mixed += dot(table_ref[base + m, 0], low_ref[...])
                yr = mixed[:TILE, :LANES] - mixed[TILE:, LANES:]
                yi = mixed[TILE:, :LANES] + mixed[:TILE, LANES:]
                here = pl.ds(pl.multiple_of((base + m) * TILE, TILE), TILE)
                cosine, sine = rc_ref[here, :], rs_ref[here, :]
                there = pl.ds(pl.multiple_of(m * TILE, TILE), TILE)
                out_ref[0, there, :] = yr * cosine - yi * sine
                out_ref[1, there, :] = yr * sine + yi * cosine
                return carry

            lax.fori_loop(0, size // TILE, tile, 0)
            base += size // TILE


def row_stage(coef, turn, scale, table, mine, theirs, slots, sizes, after):
    rows = mine[0].shape[-2]
    shapes = [jax.ShapeDtypeStruct((2, size, LANES), jnp.float32) for size in sizes for _ in slots]
    outs = pl.pallas_call(
        functools.partial(row_kernel, slots, sizes),
        in_specs=[SCALAR, ANYWHERE] + [WHOLE] * (5 + 2 * len(mine)),
        out_specs=[WHOLE] * len(shapes),
        out_shape=shapes,
        scratch_shapes=[pltpu.VMEM((rows, 2 * LANES), jnp.bfloat16)] * 2,
        cost_estimate=pl.CostEstimate(flops=len(slots) * (100 << 20), bytes_accessed=8 << 20, transcendentals=0),
        name="row_stage",
    )(coef, after, *turn, *scale, table, *mine, *theirs)
    return [outs[k * len(slots) : (k + 1) * len(slots)] for k in range(len(sizes))]


def lane_kernel(block, z_ref, jc_ref, js_ref, table_ref, *refs):
    count = jc_ref.shape[0]
    scratch = refs[-1]
    re_ref, im_ref, prob_ref = refs[-4:-1]
    for n in range(count):
        scratch[(n // SWAP) * SWAP + jnp.bitwise_xor(z_ref[0], n % SWAP)] = refs[n][...]
    reals, imags = fourier([scratch[n, 0] for n in range(count)], [scratch[n, 1] for n in range(count)])
    highs, lows = [], []
    for j in range(count):
        c, s = jc_ref[j : j + 1, :], js_ref[j : j + 1, :]
        rh, rl = halves(reals[j] * c - imags[j] * s)
        ih, il = halves(reals[j] * s + imags[j] * c)
        highs.append(jnp.concatenate([rh, ih], axis=1))
        lows.append(jnp.concatenate([rl, il], axis=1))
    high, low = jnp.concatenate(highs, axis=0), jnp.concatenate(lows, axis=0)
    dot = functools.partial(jnp.dot, preferred_element_type=jnp.float32)
    mixed = dot(high, table_ref[0]) + dot(high, table_ref[1]) + dot(low, table_ref[0])
    cube = jnp.swapaxes(mixed.reshape(count, block, 2 * LANES), 0, 1)
    re, im = cube[:, :, :LANES], cube[:, :, LANES:]
    re_ref[...] = re
    im_ref[...] = im
    prob_ref[...] = re * re + im * im


def lane_stage(z, sources, previous, start, part, rows, inner, table):
    count = inner[0].shape[0]
    block = 64
    first = start // block
    jspec = pl.BlockSpec((count, LANES), lambda i: (0, 0))
    out = pl.BlockSpec((block, count, LANES), lambda i: (first + i, 0, 0))
    shape = jax.ShapeDtypeStruct((rows, count, LANES), jnp.float32)
    arguments = [z, *inner, table]
    specs = [SCALAR, jspec, jspec, pl.BlockSpec((2, 2 * LANES, 2 * LANES), lambda i: (0, 0, 0))]
    for source, base in sources:
        offset = (start - base) // block
        arguments += source
        specs += [pl.BlockSpec((2, block, LANES), lambda i, offset=offset: (0, offset + i, 0))] * SWAP
    aliases = {}
    kernel = functools.partial(lane_kernel, block)
    if previous is not None:
        aliases = {len(arguments) + k: k for k in range(3)}
        arguments += previous
        specs += [ANYWHERE] * 3
    return pl.pallas_call(
        kernel,
        grid=(part // block,),
        in_specs=specs,
        out_specs=[out, out, out],
        out_shape=[shape, shape, shape],
        scratch_shapes=[pltpu.VMEM((count, 2, block, LANES), jnp.float32)],
        input_output_aliases=aliases,
        cost_estimate=pl.CostEstimate(
            flops=20 * count * part * LANES * LANES, bytes_accessed=20 * count * part * LANES, transcendentals=0
        ),
        name="lane_stage",
    )(*arguments)


def on_device(state_re, state_im):
    devices = lax.axis_size(AXES)
    sizes = [lax.axis_size(axis) for axis in AXES]
    assert sizes[0] == 2 and sizes[1] == 2 and sizes[2] % SWAP == 0
    weights = sizes[2] // SWAP
    local = state_re.shape[0]
    total = devices * local
    inside = SLICES * SWAP
    rows = local // (inside * LANES)
    x, core, g = (lax.axis_index(axis).astype(jnp.int32) for axis in AXES)
    z, w = g // weights, g % weights
    zs = z.reshape(1)
    rev_a, rev_l, rev_z = reversed_bits(rows), reversed_bits(LANES), reversed_bits(SWAP)
    places = jnp.arange(SWAP, dtype=jnp.int32)
    slots = jnp.bitwise_xor(places, z)
    a_index = jnp.arange(rows, dtype=jnp.int32)
    w_bits = weights.bit_length() - 1
    rev_w = sum(((w >> t) & 1) << (w_bits - 1 - t) for t in range(w_bits))

    def flip(values, distance):
        return lax.ppermute(values, AXES, [(i, i ^ distance) for i in range(devices)])

    def coefficients(bit, exponents, modulus):
        c, s = phases(bit * exponents, modulus)
        sign = (1 - 2 * bit).astype(jnp.float32).reshape(1)
        return jnp.concatenate([c, s, sign])

    x_coef = coefficients(x, core * (devices // 4) + slots * weights + w, devices)
    core_coef = coefficients(core, places * weights + w, devices // 2)
    z_turn = jnp.concatenate(phases(rev_z * w, SWAP * weights))
    w_coef = {t: coefficients((w >> t) & 1, 0 * places + w % (1 << t), 2 << t) for t in range(w_bits)}
    low_k = x + 2 * core + 16 * rev_w
    k_slot = low_k + 4 * (2 * (slots & 1) + (slots >> 1))
    k_here = low_k + 4 * (2 * (z & 1) + (z >> 1))

    cosine, sine = phases(rev_a[:, None] * a_index[None, :], rows)
    tiles = (rows // TILE, TILE, rows)
    table = jnp.concatenate([cosine.reshape(tiles), sine.reshape(tiles)], axis=1)
    row_table = jnp.stack(table_halves(table), axis=1)
    offsets = jnp.arange(SLICES, dtype=jnp.int32) * SWAP + z
    turns = [
        phases((a_index[:, None] * (inside * LANES) + offsets[c] * LANES) * k_slot[None, :], total)
        for c in range(SLICES)
    ]

    lane = np.arange(LANES, dtype=np.int32)
    scales = [
        phases(rev_a[:, None] * (offsets[c] * LANES + lane[None, :]), rows * inside * LANES) for c in range(SLICES)
    ]
    k_inner = reversed_bits(inside)[:, None] * (devices * rows)
    inner = phases((k_here + k_inner) * lane[None, :], total)
    angle = (lane[:, None] * rev_l[None, :] % LANES) * (2.0 * math.pi / LANES)
    c, s = np.cos(angle) / math.sqrt(total), np.sin(angle) / math.sqrt(total)
    lane_table = jnp.stack(table_halves(jnp.asarray(np.block([[c, s], [-s, c]]), jnp.float32)))

    re, im = (v.reshape(rows, inside, LANES) for v in (state_re, state_im))
    chain = [zs]

    def kernel(function, *arguments):
        result = function(*arguments, chain[0])
        leaf = jax.tree.leaves(result)[0]
        chain[0] = leaf
        return result

    def swap_out(arrays):
        return [arrays[0]] + [flip(arrays[s], s * weights) for s in range(1, SWAP)]

    packed, inward, across, mixed, spread = {}, {}, {}, {}, {}
    parts = {k: (rows,) for k in range(SLICES)}
    parts[SLICES - 1] = (rows // 2, rows // 4, rows // 4)
    outward = {k: [[None] * SWAP for _ in sizes] for k, sizes in parts.items()}

    def pack(k, *after):
        packed[k] = pack_stage(zs, re, im, k, [chain[0], *after])
        chain[0] = packed[k][0]
        inward[k] = swap_out(packed[k])
        across[k] = [flip(packed[k][0], devices // 2)]

    def cross(k):
        across[k] += [flip(v, devices // 2) for v in inward[k][1:]]

    def mixing(k):
        (mixed[k],) = kernel(mix_stage, x_coef, inward[k], across[k], False)
        spread[k] = flip(mixed[k], devices // 4)

    def swapping(k):
        mixed[k] = kernel(swap_stage, zs, core_coef, z_turn, mixed[k], spread[k], True)
        for t in range(w_bits - 1, -1, -1):
            spread[k] = [None] * SWAP
            for s in sum(GROUPS, ()):
                spread[k][s] = flip(mixed[k][s], 1 << t)
            if t:
                mixed[k] = kernel(mix_stage, w_coef[t], mixed[k], spread[k], True)

    def finish(k, n):
        mine, theirs = ([v[k][s] for s in GROUPS[n]] for v in (mixed, spread))
        shared = (w_coef[0], turns[k], scales[k], row_table)
        pieces = kernel(row_stage, *shared, mine, theirs, GROUPS[n], parts[k])
        for p, piece in enumerate(pieces):
            for s, value in zip(GROUPS[n], piece):
                outward[k][p][s] = flip(value, s * weights) if s else value

    pack(0), pack(1, row_table, *scales[0], *turns[0]), pack(2), pack(3)
    cross(0), cross(1), mixing(0), swapping(0), mixing(1), swapping(1)
    finish(0, 0), cross(2), finish(0, 1), cross(3), finish(1, 0), mixing(2), swapping(2), finish(1, 1)
    mixing(3), finish(2, 0), swapping(3), finish(2, 1), finish(3, 0), finish(3, 1)
    outs, start, last = None, 0, SLICES - 1
    for n, part in enumerate(parts[last]):
        sources = [(outward[k][0], 0) for k in range(last)] + [(outward[last][n], start)]
        outs = lane_stage(zs, sources, outs, start, part, rows, inner, lane_table)
        start += part
    return tuple(values.reshape(local) for values in outs)


def solution(mesh):
    spec = P(AXES)
    return jax.shard_map(
        on_device, mesh=mesh, in_specs=(spec, spec), out_specs=(spec, spec, spec), check_vma=False
    )
```

```python
import functools
import math

import jax
import jax.numpy as jnp
import numpy as np
from jax import lax
from jax.experimental import pallas as pl
from jax.experimental.pallas import tpu as pltpu
from jax.sharding import PartitionSpec as P


AXES = ("gx", "gy", "gz")
LANES = 128
SLICES = 4
SWAP = 4
TILE = 128
GROUPS = ((2, 3), (1, 0))

FULL = pltpu.CompilerParams(vmem_limit_bytes=67043328)
SCALAR = pl.BlockSpec(memory_space=pltpu.SMEM)
ANYWHERE = pl.BlockSpec(memory_space=pl.ANY)
WHOLE = pl.BlockSpec(memory_space=pltpu.VMEM)


def reversed_bits(count):
    bits = count.bit_length() - 1
    values = np.arange(count)
    result = np.zeros(count, np.int32)
    for place in range(bits):
        result += ((values >> place) & 1) << (bits - 1 - place)
    return result.astype(np.int32)


def phases(product, modulus):
    angle = (product % modulus).astype(jnp.float32) * (2.0 * math.pi / modulus)
    return jnp.cos(angle), jnp.sin(angle)


def halves(values):
    high = values.astype(jnp.bfloat16)
    low = (values - high.astype(jnp.float32)).astype(jnp.bfloat16)
    return high, low


def table_halves(values):
    high = lax.reduce_precision(values, 8, 7)
    return high.astype(jnp.bfloat16), (values - high).astype(jnp.bfloat16)


def fourier(reals, imags):
    count = len(reals)
    span = count // 2
    reals, imags = list(reals), list(imags)
    while span >= 1:
        for start in range(0, count, 2 * span):
            for offset in range(span):
                top, bottom = start + offset, start + offset + span
                ar, ai, br, bi = reals[top], imags[top], reals[bottom], imags[bottom]
                reals[top], imags[top] = ar + br, ai + bi
                dr, di = ar - br, ai - bi
                if offset == 0:
                    reals[bottom], imags[bottom] = dr, di
                elif 2 * offset == span:
                    reals[bottom], imags[bottom] = -di, dr
                else:
                    angle = math.pi * offset / span
                    c, s = math.cos(angle), math.sin(angle)
                    if 4 * offset == span:
                        reals[bottom], imags[bottom] = (dr - di) * c, (dr + di) * c
                    elif 4 * offset == 3 * span:
                        reals[bottom], imags[bottom] = -(dr + di) * s, (dr - di) * s
                    else:
                        reals[bottom], imags[bottom] = dr * c - di * s, dr * s + di * c
        span //= 2
    return reals, imags


def pack_kernel(first, slots, z_ref, re_ref, im_ref, *refs):
    outs = refs[-len(slots) :]
    block, tile, lanes = re_ref.shape
    for side, ref in enumerate((re_ref, im_ref)):
        flat = ref.reshape(block * tile, lanes)
        for slot, out_ref in zip(slots, outs):
            place = first + jnp.bitwise_xor(z_ref[0], slot)
            out_ref[side] = flat[pl.ds(place, block, stride=tile), :]


def pack_stage(z, re, im, c, slots, after):
    rows, _, lanes = re.shape
    block, tile = 256, 8
    spec = pl.BlockSpec((block, tile, lanes), lambda i: (i, c * SWAP // tile, 0))
    out = pl.BlockSpec((2, block, lanes), lambda i: (0, i, 0))
    return pl.pallas_call(
        functools.partial(pack_kernel, c * SWAP % tile, slots),
        grid=(rows // block,),
        in_specs=[SCALAR, spec, spec] + [ANYWHERE] * len(after),
        out_specs=[out] * len(slots),
        out_shape=[jax.ShapeDtypeStruct((2, rows, lanes), jnp.float32)] * len(slots),
        cost_estimate=pl.CostEstimate(flops=40 << 20, bytes_accessed=8 << 20, transcendentals=0),
        name="pack_stage",
    )(z, re, im, *after)


def butterfly(mine, theirs, sign, cosine, sine):
    r, i = theirs[0] + sign * mine[0], theirs[1] + sign * mine[1]
    return r * cosine - i * sine, r * sine + i * cosine


def per_slot(refs):
    return [refs[0].at[s] for s in range(SWAP)] if len(refs) == 1 else refs


def slot_spec(listed, block):
    if listed:
        return [pl.BlockSpec((2, block, LANES), lambda i: (0, i, 0))] * SWAP
    return [pl.BlockSpec((SWAP, 2, block, LANES), lambda i: (0, 0, i, 0))]


def slot_shape(listed, rows):
    shape = (2, rows, LANES) if listed else (SWAP, 2, rows, LANES)
    return [jax.ShapeDtypeStruct(shape, jnp.float32)] * (SWAP if listed else 1)


def mix_kernel(inputs, coef_ref, after_ref, *refs):
    mine, theirs, outs = (
        per_slot(part) for part in (refs[:inputs], refs[inputs : 2 * inputs], refs[2 * inputs :])
    )
    for s in range(SWAP):
        r, i = butterfly(mine[s], theirs[s], coef_ref[2 * SWAP], coef_ref[s], coef_ref[SWAP + s])
        outs[s][0], outs[s][1] = r, i


def mix_stage(coef, mine, theirs, listed, after):
    rows = mine[0].shape[-2]
    block = 256
    return pl.pallas_call(
        functools.partial(mix_kernel, len(mine)),
        grid=(rows // block,),
        in_specs=[SCALAR, ANYWHERE] + slot_spec(len(mine) > 1, block) * 2,
        out_specs=slot_spec(listed, block),
        out_shape=slot_shape(listed, rows),
        cost_estimate=pl.CostEstimate(flops=20 << 20, bytes_accessed=6 << 20, transcendentals=0),
        compiler_params=FULL,
        name="mix_stage",
    )(coef, after, *mine, *theirs)


def swap_kernel(z_ref, coef_ref, turn_ref, after_ref, mine_ref, theirs_ref, *refs):
    outs, scratch = per_slot(refs[:-1]), refs[-1]
    reals, imags = [], []
    for place in range(SWAP):
        slot = jnp.bitwise_xor(z_ref[0], place)
        r, i = butterfly(
            mine_ref.at[slot], theirs_ref.at[slot], coef_ref[2 * SWAP], coef_ref[place], coef_ref[SWAP + place]
        )
        reals.append(r)
        imags.append(i)
    reals, imags = fourier(reals, imags)
    for place in range(SWAP):
        c, s = turn_ref[place], turn_ref[SWAP + place]
        scratch[place, 0] = reals[place] * c - imags[place] * s
        scratch[place, 1] = reals[place] * s + imags[place] * c
    for slot in range(SWAP):
        outs[slot][...] = scratch[jnp.bitwise_xor(z_ref[0], slot)]


def swap_stage(z, coef, turn, mine, theirs, listed, after):
    rows = mine.shape[-2]
    block = 256
    full = slot_spec(False, block)
    return pl.pallas_call(
        swap_kernel,
        grid=(rows // block,),
        in_specs=[SCALAR, SCALAR, SCALAR, ANYWHERE] + full * 2,
        out_specs=slot_spec(listed, block),
        out_shape=slot_shape(listed, rows),
        scratch_shapes=[pltpu.VMEM((SWAP, 2, block, LANES), jnp.float32)],
        cost_estimate=pl.CostEstimate(flops=30 << 20, bytes_accessed=6 << 20, transcendentals=0),
        compiler_params=FULL,
        name="swap_stage",
    )(z, coef, turn, after, mine, theirs)


def row_kernel(slots, sizes, coef_ref, after_ref, tc_ref, ts_ref, rc_ref, rs_ref, table_ref, *refs):
    refs, (high_ref, low_ref) = refs[:-2], refs[-2:]
    inputs = len(slots) if len(slots) < SWAP else 1
    mine, theirs, outs = refs[:inputs], refs[inputs : 2 * inputs], refs[2 * inputs :]
    if len(slots) == SWAP:
        mine, theirs = per_slot(mine), per_slot(theirs)
    dot = functools.partial(jnp.dot, preferred_element_type=jnp.float32)
    for n, s in enumerate(slots):
        r, i = butterfly(mine[n], theirs[n], coef_ref[2 * SWAP], coef_ref[0], coef_ref[SWAP])
        cosine, sine = tc_ref[:, s : s + 1], ts_ref[:, s : s + 1]
        high_ref[:, :LANES], low_ref[:, :LANES] = halves(r * cosine - i * sine)
        high_ref[:, LANES:], low_ref[:, LANES:] = halves(r * sine + i * cosine)
        base = 0
        for part, size in enumerate(sizes):
            out_ref = outs[part * len(slots) + n]

            def tile(m, carry, out_ref=out_ref, base=base):
                high = high_ref[...]
                mixed = dot(table_ref[base + m, 0], high) + dot(table_ref[base + m, 1], high)
                mixed += dot(table_ref[base + m, 0], low_ref[...])
                yr = mixed[:TILE, :LANES] - mixed[TILE:, LANES:]
                yi = mixed[TILE:, :LANES] + mixed[:TILE, LANES:]
                here = pl.ds(pl.multiple_of((base + m) * TILE, TILE), TILE)
                cosine, sine = rc_ref[here, :], rs_ref[here, :]
                there = pl.ds(pl.multiple_of(m * TILE, TILE), TILE)
                out_ref[0, there, :] = yr * cosine - yi * sine
                out_ref[1, there, :] = yr * sine + yi * cosine
                return carry

            lax.fori_loop(0, size // TILE, tile, 0)
            base += size // TILE


def row_stage(coef, turn, scale, table, mine, theirs, slots, sizes, after):
    rows = mine[0].shape[-2]
    shapes = [jax.ShapeDtypeStruct((2, size, LANES), jnp.float32) for size in sizes for _ in slots]
    outs = pl.pallas_call(
        functools.partial(row_kernel, slots, sizes),
        in_specs=[SCALAR, ANYWHERE] + [WHOLE] * (5 + 2 * len(mine)),
        out_specs=[WHOLE] * len(shapes),
        out_shape=shapes,
        scratch_shapes=[pltpu.VMEM((rows, 2 * LANES), jnp.bfloat16)] * 2,
        cost_estimate=pl.CostEstimate(flops=len(slots) * (100 << 20), bytes_accessed=8 << 20, transcendentals=0),
        compiler_params=FULL,
        name="row_stage",
    )(coef, after, *turn, *scale, table, *mine, *theirs)
    return [outs[k * len(slots) : (k + 1) * len(slots)] for k in range(len(sizes))]


def lane_kernel(block, z_ref, jc_ref, js_ref, table_ref, *refs):
    count = jc_ref.shape[0]
    scratch = refs[-1]
    re_ref, im_ref, prob_ref = refs[-4:-1]
    for n in range(count):
        scratch[(n // SWAP) * SWAP + jnp.bitwise_xor(z_ref[0], n % SWAP)] = refs[n][...]
    reals, imags = fourier([scratch[n, 0] for n in range(count)], [scratch[n, 1] for n in range(count)])
    highs, lows = [], []
    for j in range(count):
        c, s = jc_ref[j : j + 1, :], js_ref[j : j + 1, :]
        rh, rl = halves(reals[j] * c - imags[j] * s)
        ih, il = halves(reals[j] * s + imags[j] * c)
        highs.append(jnp.concatenate([rh, ih], axis=1))
        lows.append(jnp.concatenate([rl, il], axis=1))
    high, low = jnp.concatenate(highs, axis=0), jnp.concatenate(lows, axis=0)
    dot = functools.partial(jnp.dot, preferred_element_type=jnp.float32)
    mixed = dot(high, table_ref[0]) + dot(high, table_ref[1]) + dot(low, table_ref[0])
    cube = jnp.swapaxes(mixed.reshape(count, block, 2 * LANES), 0, 1)
    re, im = cube[:, :, :LANES], cube[:, :, LANES:]
    re_ref[...] = re
    im_ref[...] = im
    prob_ref[...] = re * re + im * im


def lane_stage(z, sources, previous, start, part, rows, inner, table):
    count = inner[0].shape[0]
    block = 64
    first = start // block
    jspec = pl.BlockSpec((count, LANES), lambda i: (0, 0))
    out = pl.BlockSpec((block, count, LANES), lambda i: (first + i, 0, 0))
    shape = jax.ShapeDtypeStruct((rows, count, LANES), jnp.float32)
    arguments = [z, *inner, table]
    specs = [SCALAR, jspec, jspec, pl.BlockSpec((2, 2 * LANES, 2 * LANES), lambda i: (0, 0, 0))]
    for source, base in sources:
        offset = (start - base) // block
        arguments += source
        specs += [pl.BlockSpec((2, block, LANES), lambda i, offset=offset: (0, offset + i, 0))] * SWAP
    aliases = {}
    kernel = functools.partial(lane_kernel, block)
    if previous is not None:
        aliases = {len(arguments) + k: k for k in range(3)}
        arguments += previous
        specs += [ANYWHERE] * 3
    return pl.pallas_call(
        kernel,
        grid=(part // block,),
        in_specs=specs,
        out_specs=[out, out, out],
        out_shape=[shape, shape, shape],
        scratch_shapes=[pltpu.VMEM((count, 2, block, LANES), jnp.float32)],
        input_output_aliases=aliases,
        cost_estimate=pl.CostEstimate(
            flops=20 * count * part * LANES * LANES, bytes_accessed=20 * count * part * LANES, transcendentals=0
        ),
        compiler_params=FULL,
        name="lane_stage",
    )(*arguments)


def on_device(state_re, state_im):
    devices = lax.axis_size(AXES)
    sizes = [lax.axis_size(axis) for axis in AXES]
    assert sizes[0] == 2 and sizes[1] == 2 and sizes[2] % SWAP == 0
    weights = sizes[2] // SWAP
    local = state_re.shape[0]
    total = devices * local
    inside = SLICES * SWAP
    rows = local // (inside * LANES)
    x, core, g = (lax.axis_index(axis).astype(jnp.int32) for axis in AXES)
    z, w = g // weights, g % weights
    zs = z.reshape(1)
    rev_a, rev_l, rev_z = reversed_bits(rows), reversed_bits(LANES), reversed_bits(SWAP)
    places = jnp.arange(SWAP, dtype=jnp.int32)
    slots = jnp.bitwise_xor(places, z)
    a_index = jnp.arange(rows, dtype=jnp.int32)
    w_bits = weights.bit_length() - 1
    rev_w = sum(((w >> t) & 1) << (w_bits - 1 - t) for t in range(w_bits))

    def flip(values, distance):
        return lax.ppermute(values, AXES, [(i, i ^ distance) for i in range(devices)])

    def coefficients(bit, exponents, modulus):
        c, s = phases(bit * exponents, modulus)
        sign = (1 - 2 * bit).astype(jnp.float32).reshape(1)
        return jnp.concatenate([c, s, sign])

    x_coef = coefficients(x, core * (devices // 4) + slots * weights + w, devices)
    core_coef = coefficients(core, places * weights + w, devices // 2)
    z_turn = jnp.concatenate(phases(rev_z * w, SWAP * weights))
    w_coef = {t: coefficients((w >> t) & 1, 0 * places + w % (1 << t), 2 << t) for t in range(w_bits)}
    low_k = x + 2 * core + 16 * rev_w
    k_slot = low_k + 4 * (2 * (slots & 1) + (slots >> 1))
    k_here = low_k + 4 * (2 * (z & 1) + (z >> 1))

    cosine, sine = phases(rev_a[:, None] * a_index[None, :], rows)
    tiles = (rows // TILE, TILE, rows)
    table = jnp.concatenate([cosine.reshape(tiles), sine.reshape(tiles)], axis=1)
    row_table = jnp.stack(table_halves(table), axis=1)
    offsets = jnp.arange(SLICES, dtype=jnp.int32) * SWAP + z
    turns = [
        phases((a_index[:, None] * (inside * LANES) + offsets[c] * LANES) * k_slot[None, :], total)
        for c in range(SLICES)
    ]

    lane = np.arange(LANES, dtype=np.int32)
    scales = [
        phases(rev_a[:, None] * (offsets[c] * LANES + lane[None, :]), rows * inside * LANES) for c in range(SLICES)
    ]
    k_inner = reversed_bits(inside)[:, None] * (devices * rows)
    inner = phases((k_here + k_inner) * lane[None, :], total)
    angle = (lane[:, None] * rev_l[None, :] % LANES) * (2.0 * math.pi / LANES)
    c, s = np.cos(angle) / math.sqrt(total), np.sin(angle) / math.sqrt(total)
    lane_table = jnp.stack(table_halves(jnp.asarray(np.block([[c, s], [-s, c]]), jnp.float32)))

    re, im = (v.reshape(rows, inside, LANES) for v in (state_re, state_im))
    chain = [zs]

    def kernel(function, *arguments):
        result = function(*arguments, chain[0])
        leaf = jax.tree.leaves(result)[0]
        chain[0] = leaf
        return result

    packed, inward, across, mixed, spread = {}, {}, {}, {}, {}
    parts = {k: (rows,) for k in range(SLICES)}
    parts[SLICES - 1] = (rows // 2, rows // 4, rows // 4)
    outward = {k: [[None] * SWAP for _ in sizes] for k, sizes in parts.items()}

    def pack(k, *after):
        packed[k], inward[k] = [None] * SWAP, [None] * SWAP
        for group in GROUPS if k == 0 else (sum(GROUPS, ()),):
            pieces = pack_stage(zs, re, im, k, group, [chain[0], *after])
            chain[0] = pieces[0]
            for s, piece in zip(group, pieces):
                packed[k][s] = piece
                inward[k][s] = flip(piece, s * weights) if s else piece
        across[k] = [flip(packed[k][0], devices // 2)]

    def cross(k):
        across[k] += [flip(v, devices // 2) for v in inward[k][1:]]

    def mixing(k):
        (mixed[k],) = kernel(mix_stage, x_coef, inward[k], across[k], False)
        spread[k] = flip(mixed[k], devices // 4)

    def swapping(k):
        mixed[k] = kernel(swap_stage, zs, core_coef, z_turn, mixed[k], spread[k], True)
        for t in range(w_bits - 1, -1, -1):
            spread[k] = [None] * SWAP
            for s in sum(GROUPS, ()):
                spread[k][s] = flip(mixed[k][s], 1 << t)
            if t:
                mixed[k] = kernel(mix_stage, w_coef[t], mixed[k], spread[k], True)

    def finish(k, n):
        mine, theirs = ([v[k][s] for s in GROUPS[n]] for v in (mixed, spread))
        shared = (w_coef[0], turns[k], scales[k], row_table)
        pieces = kernel(row_stage, *shared, mine, theirs, GROUPS[n], parts[k])
        for p, piece in enumerate(pieces):
            for s, value in zip(GROUPS[n], piece):
                outward[k][p][s] = flip(value, s * weights) if s else value

    pack(0), pack(1, row_table, *scales[0], *turns[0]), pack(2), pack(3)
    cross(0), cross(1), mixing(0), swapping(0), mixing(1), swapping(1)
    finish(0, 0), cross(2), finish(0, 1), cross(3), finish(1, 0), mixing(2), swapping(2), finish(1, 1)
    mixing(3), finish(2, 0), swapping(3), finish(2, 1), finish(3, 0), finish(3, 1)
    outs, start, last = None, 0, SLICES - 1
    for n, part in enumerate(parts[last]):
        sources = [(outward[k][0], 0) for k in range(last)] + [(outward[last][n], start)]
        outs = lane_stage(zs, sources, outs, start, part, rows, inner, lane_table)
        start += part
    return tuple(values.reshape(local) for values in outs)


def solution(mesh):
    spec = P(AXES)
    return jax.shard_map(
        on_device, mesh=mesh, in_specs=(spec, spec), out_specs=(spec, spec, spec), check_vma=False
    )
```
